128 devices in a mesh: rows: 128 (over x, z, y, core).
Axes of the slice: x: 4, y: 4, z: 4, core: 2. Of those that a mesh axis runs over, the one named last changes fastest.
Arguments:
- tile_values: float32 [26624, 128, 128], P('rows'), as said below
- tile_row: int32 [26624], P('rows'), may hold values from 0 to 15, as said below
- tile_slot: int32 [26624], P('rows'), may hold values from 0 to 143, as said below
- tile_count: int32 [128], P('rows'), may hold values from 144 to 208, as said below
- requests: int32 [128, 128, 1], P('rows'), may hold values from 0 to 15
- right_side: float32 [2048, 4, 128], P('rows')
Outputs:
- solution: float32 [2048, 4, 128], P('rows')
- hessenberg: float32 [4, 4, 3], replicated
The draws below stay inside these ranges and needn't reach their ends.
Inputs may be any that keep to these rules, and one draw needn't show every extreme that they name: `tile_row`: tile t < 16 of every device lies in block row t; it is the diagonal tile of that row. `tile_slot`: slot s < 16 is the device's own block s; slot 16 + o + q is the q-th block requested from device o; tile t < 144 of every device uses slot t. `tile_count`: some device uses all 208 slots. requests[d, o, q] is a block index among device o's 16 block rows. `tile_values`: tile t < 16 of every device holds the diagonal block of its row.
All inputs are finite; a program needn't handle non-finite values.
Results may differ from the reference program's by a relative error of at most 0.0003.
Values sent between devices are 32-bit elements; how exact they have to be, the bound alone decides.
A program may use at most 64 MiB of HBM per device.

```python
import jax
import jax.numpy as jnp
from jax import lax

BS = 128
RB = 16
NRHS = 4
REQ = 1
EXTRA = 64
ITERS = 3
BLOCKS = 2048
SLOTS = 144
TILES_DEV = 208
NTILES = 26624
N_ROWS = 128


def draw_tile_values(key, part):
    position = jnp.arange(NTILES, dtype=jnp.int32)
    diagonal_tile = position % TILES_DEV < RB
    spread = 0.7 / jnp.sqrt(jnp.float32(BS * TILES_DEV / RB))
    noise_key = jax.random.fold_in(key, 11)
    scale_key = jax.random.fold_in(key, 12)
    noise = jax.random.normal(noise_key, (NTILES, BS, BS), jnp.float32)
    scales = jax.random.uniform(scale_key, (NTILES, BS), jnp.float32, 1.0, 2.0)
    boosted = jnp.where(diagonal_tile[:, None], scales, 0.0)
    identity = jnp.eye(BS, dtype=jnp.float32)
    return noise * spread + boosted[:, :, None] * identity[None, :, :]


def draw_tile_row(key, part):
    position = jnp.arange(NTILES, dtype=jnp.int32) % TILES_DEV
    chosen = jax.random.randint(jax.random.fold_in(key, 21), (NTILES,), 0, RB, dtype=jnp.int32)
    return jnp.where(position < RB, position, chosen).astype(jnp.int32)


def draw_tile_slot(key, part):
    position = jnp.arange(NTILES, dtype=jnp.int32) % TILES_DEV
    chosen = jax.random.randint(jax.random.fold_in(key, 31), (NTILES,), 0, SLOTS, dtype=jnp.int32)
    return jnp.where(position < SLOTS, position, chosen).astype(jnp.int32)


def draw_tile_count(key, part):
    devices = NTILES // TILES_DEV
    level = jax.random.randint(jax.random.fold_in(key, 41), (devices,), 0, 65, dtype=jnp.int32)
    counts = SLOTS + EXTRA * level * level // 4096
    busiest = jax.random.randint(jax.random.fold_in(key, 42), (), 0, devices, dtype=jnp.int32)
    return jnp.where(jnp.arange(devices, dtype=jnp.int32) == busiest, TILES_DEV, counts).astype(jnp.int32)


def draw_right_side(key, part):
    devices = BLOCKS // RB
    owner_of = (jnp.arange(BLOCKS, dtype=jnp.int32) // RB).astype(jnp.float32)
    ramp = 1.0 + 2.0 * owner_of / max(devices - 1, 1)
    rough = jnp.exp(jax.random.uniform(jax.random.fold_in(key, 51), (BLOCKS, NRHS, 1), jnp.float32, -0.7, 0.7))
    values = jax.random.normal(jax.random.fold_in(key, 52), (BLOCKS, NRHS, BS), jnp.float32)
    return values * rough * ramp[:, None, None]


def set_ends(result, stream_key, low, high):
    place = [jax.random.randint(jax.random.fold_in(stream_key, axis), (), 0, length) for axis, length in enumerate(result.shape)]
    longest = result.shape.index(max(result.shape))
    neighbour = place[:longest] + [(place[longest] + 1) % result.shape[longest]] + place[longest + 1:]
    return result.at[tuple(place)].set(low).at[tuple(neighbour)].set(high)


def setup_inputs(seed: int = 0) -> dict:
    key_of = jax.random.split(jax.random.key(seed), 7)
    return {
        "tile_values": draw_tile_values(jax.random.fold_in(key_of[6], 71), 0),
        "tile_row": draw_tile_row(jax.random.fold_in(key_of[6], 71), 0),
        "tile_slot": draw_tile_slot(jax.random.fold_in(key_of[6], 71), 0),
        "tile_count": draw_tile_count(jax.random.fold_in(key_of[6], 71), 0),
        "requests": set_ends(jax.random.randint(key_of[4], (N_ROWS, N_ROWS, REQ), 0, RB), jax.random.fold_in(key_of[4], 1), 0, RB - 1).astype(jnp.int32),
        "right_side": draw_right_side(jax.random.fold_in(key_of[6], 71), 0),
    }


epsilon = 1e-06
highest = lax.Precision.HIGHEST

def least_squares(hessenberg, beta_norm):
    krylov = hessenberg.shape[2]
    triangle = hessenberg
    target = jnp.zeros((hessenberg.shape[0], krylov + 1), jnp.float32).at[:, 0].set(beta_norm)
    cosines = []
    sine_list = []
    for column in range(krylov):
        column_vals = triangle[:, :, column]
        for earlier in range(column):
            first_entry = column_vals[:, earlier]
            second = column_vals[:, earlier + 1]
            column_vals = column_vals.at[:, earlier].set(cosines[earlier] * first_entry + sine_list[earlier] * second)
            column_vals = column_vals.at[:, earlier + 1].set(cosines[earlier] * second - sine_list[earlier] * first_entry)
        first_entry = column_vals[:, column]
        second = column_vals[:, column + 1]
        radius = jnp.sqrt(first_entry * first_entry + second * second)
        cosine = first_entry / radius
        sine_term = second / radius
        cosines.append(cosine)
        sine_list.append(sine_term)
        column_vals = column_vals.at[:, column].set(radius).at[:, column + 1].set(0.0)
        triangle = triangle.at[:, :, column].set(column_vals)
        leading = target[:, column]
        target = target.at[:, column].set(cosine * leading).at[:, column + 1].set(-sine_term * leading)
    weights = jnp.zeros((hessenberg.shape[0], krylov), jnp.float32)
    for column in reversed(range(krylov)):
        partial_sum = target[:, column] - lax.optimization_barrier(jnp.sum(triangle[:, column, column + 1:krylov] * weights[:, column + 1:], axis=1))
        weights = weights.at[:, column].set(partial_sum / triangle[:, column, column])
    return weights

def reference(tile_values, tile_row, tile_slot, tile_count, requests, right_side):
    tile_total = tile_slot.shape[0]
    position = jnp.arange(tile_total, dtype=jnp.int32)
    device = (position // TILES_DEV).astype(jnp.int32)
    shifted = jnp.maximum(tile_slot - RB, 0)
    owner_index = (shifted // REQ).astype(jnp.int32)
    within = (shifted % REQ).astype(jnp.int32)
    remote = requests[device, owner_index, within]
    columns = jnp.where(tile_slot < RB, device * RB + tile_slot, owner_index * RB + remote).astype(jnp.int32)
    rows_global = (device * RB + tile_row).astype(jnp.int32)
    live_mask = (position % TILES_DEV < tile_count[device]).astype(jnp.float32)

    def apply_matrix(vector):
        picked = vector[columns]
        products = jnp.einsum('tij,tkj->tki', tile_values, picked, precision=highest)
        products = products * live_mask[:, None, None]
        return jax.ops.segment_sum(products, rows_global, num_segments=vector.shape[0])
    beta_norm = jnp.sqrt(lax.optimization_barrier(jnp.sum(right_side * right_side, axis=(0, 2))) + epsilon)
    basis_list = [right_side / beta_norm[None, :, None]]
    hessenberg = jnp.zeros((right_side.shape[1], ITERS + 1, ITERS), jnp.float32)
    for column in range(ITERS):
        candidate = apply_matrix(basis_list[column])
        for earlier in range(column + 1):
            projection = lax.optimization_barrier(jnp.sum(candidate * basis_list[earlier], axis=(0, 2)))
            hessenberg = hessenberg.at[:, earlier, column].set(projection)
            candidate = candidate - projection[None, :, None] * basis_list[earlier]
        length = jnp.sqrt(lax.optimization_barrier(jnp.sum(candidate * candidate, axis=(0, 2))) + epsilon)
        hessenberg = hessenberg.at[:, column + 1, column].set(length)
        if column + 1 < ITERS:
            basis_list.append(candidate / length[None, :, None])
    weights = least_squares(hessenberg, beta_norm)
    stacked = jnp.stack(basis_list)
    solution = jnp.einsum('kj,jrki->rki', weights, stacked, precision=highest)
    return (solution, hessenberg)
```

```python
import jax
import jax.numpy as jnp
from jax import lax
from jax.experimental import pallas as pl
from jax.experimental.pallas import tpu as pltpu
from jax.sharding import PartitionSpec as P

MESH = pl.DeviceIdType.MESH
F32 = jnp.float32
BF16 = jnp.bfloat16
EPS = 1e-06
N = 128
RB = 16
TILES = 208
SLOTS = 144
PAIRS = TILES // 2
CHUNK = 16
CHUNKS = TILES // CHUNK
AHEAD = 6


def hops(offset):
    return sum(min(d, 4 - d) for d in ((offset // 2) % 4, (offset // 8) % 4, offset // 32))


OFFSETS = sorted(range(1, N), key=lambda o: (-hops(o), o))


def partner(me, o):
    core = (me % 2 + o % 2) % 2
    y = ((me // 2) % 4 + (o // 2) % 4) % 4
    z = ((me // 8) % 4 + (o // 8) % 4) % 4
    x = (me // 32 + o // 32) % 4
    return ((x * 4 + z) * 4 + y) * 2 + core


def kernel(
    row_s, slot_s, count_s, tiles_hbm, req_ref, b_ref,
    sol_ref, hes_ref,
    raw, wide, left, staged, send, got, ask_out, ask_in, ask_row, ask_s, last_out, last_in,
    load_sem, send_sem, recv_sem, ask_sem,
):
    me = lax.axis_index("rows")
    lane = lax.broadcasted_iota(jnp.int32, (8, 128), 1)
    sub = lax.broadcasted_iota(jnp.int32, (8, 128), 0)
    system = sub % 4
    low = sub < 4

    def load(c):
        part = pl.ds(c * CHUNK, CHUNK)
        return pltpu.make_async_copy(tiles_hbm.at[part], raw.at[part], load_sem.at[c])

    for c in range(CHUNKS):
        load(c).start()
    barrier = pltpu.get_barrier_semaphore()

    def greet(o, carry):
        pl.semaphore_signal(barrier, inc=1, device_id=((me + o) % N,), device_id_type=MESH)
        return carry

    lax.fori_loop(1, N, greet, 0)

    def split(v):
        hi = v.astype(BF16).astype(F32)
        return hi, v - hi

    def prepare(c, carry):
        load(c).wait()
        for i in range(CHUNK):
            t = raw[c * CHUNK + i].T
            hi = t.astype(BF16)
            lo = (t - hi.astype(F32)).astype(BF16)
            side = pl.ds((i % 2) * 128, 128)
            at = c * (CHUNK // 2) + i // 2
            wide[at, pl.ds(0, 128), side] = hi
            wide[at, pl.ds(128, 128), side] = lo
        return carry

    def start_sends(phase, source, target):
        for o in OFFSETS:
            to = partner(me, o)
            pltpu.make_async_remote_copy(
                src_ref=source(to), dst_ref=target.at[me], send_sem=send_sem.at[phase],
                recv_sem=recv_sem.at[phase], device_id=(to,), device_id_type=MESH,
            ).start()

    def wait_all(sem, like):
        whole = like.at[pl.ds(0, N - 1)]
        pltpu.make_async_copy(whole, whole, sem).wait()

    wide_lane = lax.broadcasted_iota(jnp.int32, (N, 1, 128), 2)
    ask_out[...] = jnp.where(wide_lane == me, req_ref[...].reshape(N, 1, 1), 0)

    lax.fori_loop(0, AHEAD, prepare, 0)
    pl.semaphore_wait(barrier, N - 1)
    start_sends(0, lambda to: ask_out.at[to], ask_in)
    ask_in[me] = ask_out[me]
    lax.fori_loop(AHEAD, CHUNKS, prepare, 0)

    def fold(v):
        return v + pltpu.roll(v, 4, 0)

    def product(u, v):
        s = fold(jnp.sum(u * v, axis=0))
        return jnp.broadcast_to(jnp.sum(s, axis=1, keepdims=True), (8, 128))

    def packed(values):
        y = jnp.zeros((8, 128), F32)
        for i, value in enumerate(values):
            y = jnp.where(lane // 16 == i, value, y)
        y = jnp.where((lane % 4 == sub), y, 0.0)
        return jnp.sum(y, axis=0, keepdims=True)

    def unpacked(total, count):
        spread = jnp.broadcast_to(total, (8, 128))
        out = []
        for i in range(count):
            picked = jnp.where(lane == i * 16 + system, spread, 0.0)
            out.append(jnp.broadcast_to(jnp.sum(picked, axis=1, keepdims=True), (8, 128)))
        return out

    def stage(vector, partial):
        for r in range(RB):
            half = (r % 2) * 4
            block = vector[r // 2][half : half + 4]
            staged[r] = jnp.concatenate([block, partial], axis=0)
            hi, lo = split(block)
            left[r] = jnp.concatenate([hi, lo], axis=0)

    def exchange(phase):
        out, into = send.at[phase], got.at[phase]

        def gather(d, carry):
            out[d] = staged[ask_s[0, d]]
            return carry

        lax.fori_loop(0, N, gather, 0, unroll=8)
        start_sends(phase + 1, lambda to: out.at[to], into)
        into[me] = out[me]

    def arrive(phase):
        into = got.at[phase]
        wait_all(recv_sem.at[phase + 1], into)

        def take(c, total):
            for i in range(16):
                d = c * 16 + i
                g = into[d]
                hi, lo = split(g[0:4])
                left[RB + d] = jnp.concatenate([hi, lo], axis=0)
                total = total + g
            return total

        total = lax.fori_loop(0, N // 16, take, jnp.zeros((5, 128), F32))
        return total[4:5]

    def pair(p, slot0, slot1, row0, row1, acc):
        x = jnp.concatenate([left[slot0], left[slot1]], axis=0).astype(BF16)
        x = jnp.concatenate([x, x], axis=1)
        r = jnp.dot(x, wide[p], preferred_element_type=F32)
        for row, value in ((row0, r[0:8, 0:128]), (row1, r[8:16, 128:256])):
            rows = jnp.full((8, 128), row, jnp.int32)
            acc = tuple(acc[q] + jnp.where(rows == q, value, 0.0) for q in range(RB))
        return acc

    def own_tiles():
        acc = []
        for p in range(RB // 2):
            x = jnp.concatenate([left[2 * p], left[2 * p + 1]], axis=0).astype(BF16)
            x = jnp.concatenate([x, x], axis=1)
            r = jnp.dot(x, wide[p], preferred_element_type=F32)
            acc += [r[0:8, 0:128], r[8:16, 128:256]]
        return tuple(acc)

    def other_tiles(acc):
        def known(c, acc):
            for i in range(16):
                p = RB // 2 + c * 16 + i
                acc = pair(p, 2 * p, 2 * p + 1, row_s[2 * p], row_s[2 * p + 1], acc)
            return acc

        def extra(c, acc):
            for i in range(16):
                p = SLOTS // 2 + c * 16 + i
                rows = [jnp.where(t < count_s[0], row_s[t], -1) for t in (2 * p, 2 * p + 1)]
                acc = pair(p, slot_s[2 * p], slot_s[2 * p + 1], rows[0], rows[1], acc)
            return acc

        acc = lax.fori_loop(0, (SLOTS - RB) // 32, known, acc)
        acc = lax.fori_loop(0, (TILES - SLOTS) // 32, extra, acc)
        acc = [fold(a) for a in acc]
        return jnp.stack([jnp.where(low, acc[2 * m], acc[2 * m + 1]) for m in range(RB // 2)])

    def apply(phase):
        exchange(phase)
        acc = own_tiles()
        total = arrive(phase)
        return total, other_tiles(acc)

    b = b_ref[...]
    first_partial = packed([product(b, b)])
    stage(b, first_partial)

    wait_all(recv_sem.at[0], ask_in)
    ask_row[...] = jnp.sum(ask_in[...], axis=0)
    to_scalar = pltpu.make_async_copy(ask_row, ask_s, ask_sem)
    to_scalar.start()
    to_scalar.wait()

    total, z = apply(0)
    (bb,) = unpacked(total, 1)
    beta = jnp.sqrt(bb + EPS)
    inverse = 1.0 / beta
    n00 = bb * inverse * inverse
    v0 = b * inverse
    t1 = z * inverse

    stage(t1, packed([product(t1, v0), product(t1, t1)]))
    total, z = apply(1)
    h00, tt = unpacked(total, 2)
    guess1 = jnp.sqrt(jnp.maximum(tt - 2.0 * h00 * h00 + h00 * h00 * n00, 0.0) + EPS)
    inverse = 1.0 / guess1
    u1 = (t1 - h00 * v0) * inverse
    t2 = (z - h00 * t1) * inverse

    stage(
        t2,
        packed([product(t2, v0), product(t2, u1), product(t2, t2), product(u1, u1), product(u1, v0)]),
    )
    total, z = apply(2)
    q0, q1, qq, m11, m01 = unpacked(total, 5)
    h10 = jnp.sqrt(guess1 * guess1 * m11 + EPS)
    rho = guess1 / h10
    v1 = u1 * rho
    t2 = t2 * rho
    z = z * rho
    d01 = rho * m01
    d11 = rho * rho * m11
    h01 = rho * q0
    x1 = rho * rho * q1
    h11 = x1 - h01 * d01
    square = (
        rho * rho * qq + h01 * h01 * n00 + h11 * h11 * d11
        - 2.0 * (h01 * h01 + h11 * x1) + 2.0 * h01 * h11 * d01
    )
    guess2 = jnp.sqrt(jnp.maximum(square, 0.0) + EPS)
    inverse = 1.0 / guess2
    u2 = (t2 - h01 * v0 - h11 * v1) * inverse
    t3 = (z - h01 * t1 - h11 * t2) * inverse

    last_out[...] = packed(
        [
            product(t3, v0), product(t3, v1), product(t3, u2), product(t3, t3),
            product(u2, u2), product(u2, v0), product(u2, v1),
        ]
    )
    start_sends(4, lambda to: last_out, last_in)
    last_in[me] = last_out[...]
    wait_all(recv_sem.at[4], last_in)
    total = jnp.sum(last_in[...], axis=0)
    p0, p1, p2, pp, m22, m02, m12 = unpacked(total, 7)
    h21 = jnp.sqrt(guess2 * guess2 * m22 + EPS)
    rho = guess2 / h21
    v2 = u2 * rho
    e02 = rho * m02
    e12 = rho * m12
    d22 = rho * rho * m22
    h02 = rho * p0
    x1 = rho * p1
    x2 = rho * rho * p2
    h12 = x1 - h02 * d01
    h22 = x2 - h02 * e02 - h12 * e12
    square = (
        rho * rho * pp + h02 * h02 * n00 + h12 * h12 * d11 + h22 * h22 * d22
        - 2.0 * (h02 * h02 + h12 * x1 + h22 * x2)
        + 2.0 * (h02 * h12 * d01 + h02 * h22 * e02 + h12 * h22 * e12)
    )
    h32 = jnp.sqrt(jnp.maximum(square, 0.0) + EPS)

    def rotation(a, c):
        radius = jnp.sqrt(a * a + c * c)
        return a / radius, c / radius, radius

    c0, s0, r00 = rotation(h00, h10)
    g0, g1 = c0 * beta, -s0 * beta
    r01 = c0 * h01 + s0 * h11
    c1, s1, r11 = rotation(c0 * h11 - s0 * h01, h21)
    g1, g2 = c1 * g1, -s1 * g1
    r02 = c0 * h02 + s0 * h12
    turned = c0 * h12 - s0 * h02
    r12 = c1 * turned + s1 * h22
    c2, s2, r22 = rotation(c1 * h22 - s1 * turned, h32)
    g2 = c2 * g2
    y2 = g2 / r22
    y1 = (g1 - r12 * y2) / r11
    y0 = (g0 - (r01 * y1 + r02 * y2)) / r00
    sol_ref[...] = y0 * v0 + y1 * v1 + y2 * v2

    table = ((h00, h01, h02), (h10, h11, h12), (None, h21, h22), (None, None, h32))
    for k in range(4):
        out = jnp.zeros((4, 3), F32)
        rows = lax.broadcasted_iota(jnp.int32, (4, 3), 0)
        columns = lax.broadcasted_iota(jnp.int32, (4, 3), 1)
        for i in range(4):
            for j in range(3):
                if table[i][j] is not None:
                    value = jnp.broadcast_to(table[i][j][k : k + 1, 0:3], (4, 3))
                    out = jnp.where((rows == i) & (columns == j), value, out)
        hes_ref[k] = out

    wait_all(send_sem.at[0], ask_out)
    for phase in range(3):
        wait_all(send_sem.at[phase + 1], send.at[phase])
    wait_all(send_sem.at[4], last_in)


def solution(mesh):
    def on_device(tile_values, tile_row, tile_slot, tile_count, requests, right_side):
        vmem = pl.BlockSpec(memory_space=pltpu.VMEM)
        smem = pl.BlockSpec(memory_space=pltpu.SMEM)
        answer, hessenberg = pl.pallas_call(
            kernel,
            out_shape=(
                jax.ShapeDtypeStruct((8, 8, 128), F32),
                jax.ShapeDtypeStruct((4, 4, 3), F32),
            ),
            in_specs=[smem, smem, smem, pl.BlockSpec(memory_space=pl.ANY), vmem, vmem],
            out_specs=(vmem, vmem),
            scratch_shapes=[
                pltpu.VMEM((TILES, 128, 128), F32),
                pltpu.VMEM((PAIRS, 256, 256), BF16),
                pltpu.VMEM((SLOTS, 8, 128), F32),
                pltpu.VMEM((RB, 5, 128), F32),
                pltpu.VMEM((3, N, 5, 128), F32),
                pltpu.VMEM((3, N, 5, 128), F32),
                pltpu.VMEM((N, 1, 128), jnp.int32),
                pltpu.VMEM((N, 1, 128), jnp.int32),
                pltpu.VMEM((1, 128), jnp.int32),
                pltpu.SMEM((1, 128), jnp.int32),
                pltpu.VMEM((1, 128), F32),
                pltpu.VMEM((N, 1, 128), F32),
                pltpu.SemaphoreType.DMA((CHUNKS,)),
                pltpu.SemaphoreType.DMA((5,)),
                pltpu.SemaphoreType.DMA((5,)),
                pltpu.SemaphoreType.DMA,
            ],
            compiler_params=pltpu.CompilerParams(
                collective_id=0, has_side_effects=True, vmem_limit_bytes=60 << 20
            ),
            name="arnoldi",
        )(
            tile_row, tile_slot, tile_count, tile_values,
            requests.reshape(N, 1), right_side.reshape(8, 8, 128),
        )
        return answer.reshape(RB, 4, 128), hessenberg

    rows = P("rows")
    return jax.shard_map(
        on_device,
        mesh=mesh,
        in_specs=(rows, rows, rows, rows, rows, rows),
        out_specs=(rows, P()),
        check_vma=False,
    )
```

```python
import jax
import jax.numpy as jnp
from jax import lax
from jax.experimental import pallas as pl
from jax.experimental.pallas import tpu as pltpu
from jax.sharding import PartitionSpec as P

MESH = pl.DeviceIdType.MESH
F32 = jnp.float32
BF16 = jnp.bfloat16
EPS = 1e-06
N = 128
RB = 16
TILES = 208
SLOTS = 144
PAIRS = TILES // 2
CHUNK = 16
CHUNKS = TILES // CHUNK
AHEAD = 6
FAR = 4
ROWS_AHEAD = 32


def hops(offset):
    return sum(min(d, 4 - d) for d in ((offset // 2) % 4, (offset // 8) % 4, offset // 32))


OFFSETS = sorted(range(1, N), key=lambda o: (-hops(o), o))
CHIPS = sorted(range(0, N, 2), key=lambda o: (hops(o), o))
GROUPS = ([o for o in CHIPS if hops(o) < FAR], [o for o in CHIPS if hops(o) >= FAR])
COUNTS = (2 * len(GROUPS[0]) - 1, 2 * len(GROUPS[1]))


def partners(me):
    def turned(step, size):
        digit = lax.rem(lax.div(me, step), size)
        return [lax.rem(digit + k, size) * step for k in range(size)]

    cores, y, z, x = turned(1, 2), turned(2, 4), turned(8, 4), turned(32, 4)
    return lambda o: cores[o % 2] + (y[o // 2 % 4] + (z[o // 8 % 4] + x[o // 32]))


def kernel(
    count_s, row_hbm, slot_hbm, tiles_hbm, req_hbm, b_hbm,
    sol_ref, hes_ref,
    row_s, slot_s, req_ref, b_ref,
    raw, wide, left, staged, send, got, ask_out, ask_in, ask_row, ask_s, last_out, last_in,
    load_sem, small_sem, send_sem, recv_sem, ask_sem,
):
    me = lax.axis_index("rows")
    partner = partners(me)
    lane = lax.broadcasted_iota(jnp.int32, (8, 128), 1)
    sub = lax.broadcasted_iota(jnp.int32, (8, 128), 0)
    block = lax.broadcasted_iota(jnp.int32, (RB, 8, 128), 0)
    system = sub % 4
    low = sub < 4

    def load(c):
        part = pl.ds(c * CHUNK, CHUNK)
        return pltpu.make_async_copy(tiles_hbm.at[part], raw.at[part], load_sem.at[c])

    small = [
        pltpu.make_async_copy(source, target, small_sem.at[i])
        for i, (source, target) in enumerate(
            ((req_hbm, req_ref), (b_hbm, b_ref), (row_hbm, row_s), (slot_hbm, slot_s))
        )
    ]
    for copy in small:
        copy.start()
    for c in range(CHUNKS):
        load(c).start()
    barrier = pltpu.get_barrier_semaphore()
    for o in OFFSETS:
        pl.semaphore_signal(barrier, inc=1, device_id=(partner(o),), device_id_type=MESH)
    for copy in small:
        copy.wait()

    def split(v):
        hi = v.astype(BF16).astype(F32)
        return hi, v - hi

    def prepare(c, carry):
        load(c).wait()
        for i in range(CHUNK):
            t = raw[c * CHUNK + i].T
            hi = t.astype(BF16)
            lo = (t - hi.astype(F32)).astype(BF16)
            side = pl.ds((i % 2) * 128, 128)
            at = c * (CHUNK // 2) + i // 2
            wide[at, pl.ds(0, 128), side] = hi
            wide[at, pl.ds(128, 128), side] = lo
        return carry

    def start_send(phase, group, to, source, target):
        pltpu.make_async_remote_copy(
            src_ref=source, dst_ref=target.at[me], send_sem=send_sem.at[phase],
            recv_sem=recv_sem.at[phase, group], device_id=(to,), device_id_type=MESH,
        ).start()

    def wait_for(sem, like, count=N - 1):
        whole = like.at[pl.ds(0, count)]
        pltpu.make_async_copy(whole, whole, sem).wait()

    wide_lane = lax.broadcasted_iota(jnp.int32, (N, 128), 1)
    wanted = jnp.broadcast_to(req_ref[...], (N, 128)).T
    ask_out[...] = jnp.where(wide_lane == me, wanted, 0).reshape(N, 1, 128)

    lax.fori_loop(0, AHEAD, prepare, 0)
    pl.semaphore_wait(barrier, N - 1)
    for o in OFFSETS:
        to = partner(o)
        start_send(0, 0, to, ask_out.at[to], ask_in)
    ask_in[me] = ask_out[me]
    lax.fori_loop(AHEAD, CHUNKS, prepare, 0)

    def fold(v):
        return v + pltpu.roll(v, 4, 0)

    def product(u, v):
        s = fold(jnp.sum(u * v, axis=0))
        return jnp.broadcast_to(jnp.sum(s, axis=1, keepdims=True), (8, 128))

    def packed(values):
        y = jnp.zeros((8, 128), F32)
        for i, value in enumerate(values):
            y = jnp.where(lane // 16 == i, value, y)
        y = jnp.where((lane % 4 == sub), y, 0.0)
        return jnp.sum(y, axis=0, keepdims=True)

    def unpacked(total, count):
        spread = jnp.broadcast_to(total, (8, 128))
        out = []
        for i in range(count):
            picked = jnp.where(lane == i * 16 + system, spread, 0.0)
            out.append(jnp.broadcast_to(jnp.sum(picked, axis=1, keepdims=True), (8, 128)))
        return out

    def stage(vector, partial):
        for r in range(RB):
            half = (r % 2) * 4
            block = vector[r // 2][half : half + 4]
            staged[r] = jnp.concatenate([block, partial], axis=0)
            hi, lo = split(block)
            left[r] = jnp.concatenate([hi, lo], axis=0)

    def exchange(phase):
        out, into = send.at[phase], got.at[phase]
        targets = [partner(o) for o in OFFSETS] + [me]

        def fill(i):
            out[targets[i]] = staged[ask_s[0, targets[i]]]

        for i in range(ROWS_AHEAD):
            fill(i)
        for i, o in enumerate(OFFSETS):
            start_send(phase + 1, int(hops(o) >= FAR), targets[i], out.at[targets[i]], into)
            if i + ROWS_AHEAD < N:
                fill(i + ROWS_AHEAD)
        into[me] = staged[ask_s[0, me]]

    def times(p, x0, x1):
        x = jnp.concatenate([x0, x1], axis=0).astype(BF16)
        x = jnp.concatenate([x, x], axis=1)
        r = jnp.dot(x, wide[p], preferred_element_type=F32)
        return r[0:8, 0:128], r[8:16, 128:256]

    def add(acc, row, value):
        return acc + jnp.where(block == row, value, 0.0)

    def own_tiles():
        acc = []
        for p in range(RB // 2):
            acc += times(p, left[2 * p], left[2 * p + 1])
        return jnp.stack(acc)

    def chip_tiles(into, offset, acc):
        first = partner(offset) - lax.rem(me, 2)
        x = []
        for d in (first, first + 1):
            hi, lo = split(into[d][0:4])
            x.append(jnp.concatenate([hi, lo], axis=0))
            left[RB + d] = x[-1]
        y0, y1 = times(RB // 2 + first // 2, x[0], x[1])
        return add(add(acc, row_s[RB + first], y0), row_s[RB + first + 1], y1)

    def extra_tiles(acc):
        for p in range(SLOTS // 2, PAIRS):
            y = times(p, left[slot_s[2 * p]], left[slot_s[2 * p + 1]])
            for t, value in ((2 * p, y[0]), (2 * p + 1, y[1])):
                acc = add(acc, jnp.where(t < count_s[0], row_s[t], -1), value)
        return acc

    def apply(phase, digest):
        exchange(phase)
        into = got.at[phase]
        acc = own_tiles()
        for group in range(2):
            wait_for(recv_sem.at[phase + 1, group], into, COUNTS[group])
            if group == 1:
                total = jnp.sum(into[...], axis=0)
                coefficients = digest(total[4:5])
            for offset in GROUPS[group]:
                acc = chip_tiles(into, offset, acc)
        acc = extra_tiles(acc)
        acc = [fold(acc[r]) for r in range(RB)]
        z = jnp.stack([jnp.where(low, acc[2 * m], acc[2 * m + 1]) for m in range(RB // 2)])
        return coefficients, z

    b = b_ref[...]
    first_partial = packed([product(b, b)])
    stage(b, first_partial)

    wait_for(recv_sem.at[0, 0], ask_in)
    ask_row[...] = jnp.sum(ask_in[...], axis=0)
    to_scalar = pltpu.make_async_copy(ask_row, ask_s, ask_sem)
    to_scalar.start()
    to_scalar.wait()

    def digest0(total):
        (bb,) = unpacked(total, 1)
        beta = jnp.sqrt(bb + EPS)
        inverse = 1.0 / beta
        return beta, inverse, bb * inverse * inverse

    (beta, inverse, n00), z = apply(0, digest0)
    v0 = b * inverse
    t1 = z * inverse
    stage(t1, packed([product(t1, v0), product(t1, t1)]))

    def digest1(total):
        h00, tt = unpacked(total, 2)
        square = tt - 2.0 * h00 * h00 + h00 * h00 * n00
        guess1 = jnp.sqrt(jnp.maximum(square, 0.0) + EPS)
        return h00, guess1, 1.0 / guess1

    (h00, guess1, inverse), z = apply(1, digest1)
    u1 = (t1 - h00 * v0) * inverse
    t2 = (z - h00 * t1) * inverse
    stage(
        t2,
        packed([product(t2, v0), product(t2, u1), product(t2, t2), product(u1, u1), product(u1, v0)]),
    )

    def digest2(total):
        q0, q1, qq, m11, m01 = unpacked(total, 5)
        h10 = jnp.sqrt(guess1 * guess1 * m11 + EPS)
        rho = guess1 / h10
        d01 = rho * m01
        d11 = rho * rho * m11
        h01 = rho * q0
        x1 = rho * rho * q1
        h11 = x1 - h01 * d01
        square = (
            rho * rho * qq + h01 * h01 * n00 + h11 * h11 * d11
            - 2.0 * (h01 * h01 + h11 * x1) + 2.0 * h01 * h11 * d01
        )
        guess2 = jnp.sqrt(jnp.maximum(square, 0.0) + EPS)
        return h10, rho, d01, d11, h01, h11, guess2, 1.0 / guess2

    (h10, rho, d01, d11, h01, h11, guess2, inverse), z = apply(2, digest2)
    v1 = u1 * rho
    t2 = t2 * rho
    u2 = (t2 - h01 * v0 - h11 * v1) * inverse
    t3 = (z * rho - h01 * t1 - h11 * t2) * inverse

    last_out[...] = packed(
        [
            product(t3, v0), product(t3, v1), product(t3, u2), product(t3, t3),
            product(u2, u2), product(u2, v0), product(u2, v1),
        ]
    )
    last_in[me] = last_out[...]
    for o in OFFSETS:
        start_send(4, 0, partner(o), last_out, last_in)

    def rotation(a, c):
        radius = jnp.sqrt(a * a + c * c)
        return a / radius, c / radius, radius

    c0, s0, r00 = rotation(h00, h10)
    g0, g1 = c0 * beta, -s0 * beta
    r01 = c0 * h01 + s0 * h11
    turned1 = c0 * h11 - s0 * h01

    wait_for(recv_sem.at[4, 0], last_in)
    total = jnp.sum(last_in[...], axis=0)
    p0, p1, p2, pp, m22, m02, m12 = unpacked(total, 7)
    h21 = jnp.sqrt(guess2 * guess2 * m22 + EPS)
    rho = guess2 / h21
    v2 = u2 * rho
    e02 = rho * m02
    e12 = rho * m12
    d22 = rho * rho * m22
    h02 = rho * p0
    x1 = rho * p1
    x2 = rho * rho * p2
    h12 = x1 - h02 * d01
    h22 = x2 - h02 * e02 - h12 * e12
    square = (
        rho * rho * pp + h02 * h02 * n00 + h12 * h12 * d11 + h22 * h22 * d22
        - 2.0 * (h02 * h02 + h12 * x1 + h22 * x2)
        + 2.0 * (h02 * h12 * d01 + h02 * h22 * e02 + h12 * h22 * e12)
    )
    h32 = jnp.sqrt(jnp.maximum(square, 0.0) + EPS)

    c1, s1, r11 = rotation(turned1, h21)
    g1, g2 = c1 * g1, -s1 * g1
    r02 = c0 * h02 + s0 * h12
    turned = c0 * h12 - s0 * h02
    r12 = c1 * turned + s1 * h22
    c2, s2, r22 = rotation(c1 * h22 - s1 * turned, h32)
    g2 = c2 * g2
    y2 = g2 / r22
    y1 = (g1 - r12 * y2) / r11
    y0 = (g0 - (r01 * y1 + r02 * y2)) / r00
    sol_ref[...] = y0 * v0 + y1 * v1 + y2 * v2

    columns = ((h00, h10), (h01, h11, h21), (h02, h12, h22, h32))
    for j, column in enumerate(columns):
        out = jnp.zeros((4, 4), F32)
        for i, value in enumerate(column):
            out = jnp.where(lane[0:4, 0:4] == i, value[0:4, 0:4], out)
        hes_ref[j] = out

    wait_for(send_sem.at[0], ask_out)
    for phase in range(3):
        wait_for(send_sem.at[phase + 1], send.at[phase])
    wait_for(send_sem.at[4], last_in)


def hand_over(answer_ref, hessenberg_ref, answer_out, hessenberg_out):
    answer_out[...] = answer_ref[...]
    hessenberg_out[...] = hessenberg_ref[...]


def solution(mesh):
    def on_device(tile_values, tile_row, tile_slot, tile_count, requests, right_side):
        vmem = pl.BlockSpec(memory_space=pltpu.VMEM)
        smem = pl.BlockSpec(memory_space=pltpu.SMEM)
        hbm = pl.BlockSpec(memory_space=pltpu.HBM)
        shapes = (
            jax.ShapeDtypeStruct((8, 8, 128), F32),
            jax.ShapeDtypeStruct((3, 4, 4), F32),
        )
        answer, hessenberg = pl.pallas_call(
            kernel,
            out_shape=shapes,
            in_specs=[smem, hbm, hbm, hbm, hbm, hbm],
            out_specs=(vmem, vmem),
            scratch_shapes=[
                pltpu.SMEM((TILES,), jnp.int32),
                pltpu.SMEM((TILES,), jnp.int32),
                pltpu.VMEM((1, 128), jnp.int32),
                pltpu.VMEM((8, 8, 128), F32),
                pltpu.VMEM((TILES, 128, 128), F32),
                pltpu.VMEM((PAIRS, 256, 256), BF16),
                pltpu.VMEM((SLOTS, 8, 128), F32),
                pltpu.VMEM((RB, 5, 128), F32),
                pltpu.VMEM((3, N, 5, 128), F32),
                pltpu.VMEM((3, N, 5, 128), F32),
                pltpu.VMEM((N, 1, 128), jnp.int32),
                pltpu.VMEM((N, 1, 128), jnp.int32),
                pltpu.VMEM((1, 128), jnp.int32),
                pltpu.SMEM((1, 128), jnp.int32),
                pltpu.VMEM((1, 128), F32),
                pltpu.VMEM((N, 1, 128), F32),
                pltpu.SemaphoreType.DMA((CHUNKS,)),
                pltpu.SemaphoreType.DMA((4,)),
                pltpu.SemaphoreType.DMA((5,)),
                pltpu.SemaphoreType.DMA((5, 2)),
                pltpu.SemaphoreType.DMA,
            ],
            compiler_params=pltpu.CompilerParams(
                collective_id=0, has_side_effects=True, vmem_limit_bytes=40 << 20
            ),
            name="arnoldi",
        )(
            tile_count,
            *[
                pltpu.with_memory_space_constraint(x, pltpu.HBM)
                for x in (
                    tile_row, tile_slot, tile_values,
                    requests.reshape(1, N), right_side.reshape(8, 8, 128),
                )
            ],
        )
        answer, hessenberg = pl.pallas_call(
            hand_over,
            out_shape=shapes,
            in_specs=[vmem, vmem],
            out_specs=(vmem, vmem),
            compiler_params=pltpu.CompilerParams(vmem_limit_bytes=4 << 20),
            name="hand_over",
        )(answer, hessenberg)
        return answer.reshape(RB, 4, 128), jnp.transpose(hessenberg, (1, 2, 0))

    rows = P("rows")
    return jax.shard_map(
        on_device,
        mesh=mesh,
        in_specs=(rows, rows, rows, rows, rows, rows),
        out_specs=(rows, P()),
        check_vma=False,
    )
```

```python
import jax
import jax.numpy as jnp
from jax import lax
from jax.experimental import pallas as pl
from jax.experimental.pallas import tpu as pltpu
from jax.sharding import PartitionSpec as P

MESH = pl.DeviceIdType.MESH
F32 = jnp.float32
BF16 = jnp.bfloat16
EPS = 1e-06
N = 128
RB = 16
TILES = 208
SLOTS = 144
PAIRS = TILES // 2
CHUNK = 16
CHUNKS = TILES // CHUNK
ROWS_AHEAD = 12


def hops(offset):
    return sum(min(d, 4 - d) for d in ((offset // 2) % 4, (offset // 8) % 4, offset // 32))


OFFSETS = sorted(range(1, N), key=lambda o: (-hops(o), o))
BLOCK_ORDER = (6, 5, 4, 3, 2, 1, 0)
BLOCKS = sorted(range(1, N), key=lambda o: (BLOCK_ORDER.index(hops(o)), o))
GROUP_HOPS = ((0, 1, 2), (3, 4, 5, 6))
GROUPS = [[o for o in range(0, N, 2) if hops(o) in group] for group in GROUP_HOPS]
COUNTS = [sum(hops(o) in group for o in OFFSETS) for group in GROUP_HOPS]


def group_of(o):
    return [i for i, group in enumerate(GROUP_HOPS) if hops(o) in group][0]


def partners(me):
    def turned(step, size):
        digit = lax.rem(lax.div(me, step), size)
        return [lax.rem(digit + k, size) * step for k in range(size)]

    cores, y, z, x = turned(1, 2), turned(2, 4), turned(8, 4), turned(32, 4)
    return lambda o: cores[o % 2] + (y[o // 2 % 4] + (z[o // 8 % 4] + x[o // 32]))


def kernel(
    count_s, row_hbm, slot_hbm, tiles_hbm, req_hbm, b_hbm,
    sol_ref, hes_ref,
    row_s, slot_s, req_ref, b_ref,
    raw, wide, left, staged, send, got, ask_in, sums_out, sums_in,
    load_sem, small_sem, send_sem, recv_sem, ask_sem,
):
    me = lax.axis_index("rows")
    partner = partners(me)
    lane = lax.broadcasted_iota(jnp.int32, (8, 128), 1)
    sub = lax.broadcasted_iota(jnp.int32, (8, 128), 0)
    block = lax.broadcasted_iota(jnp.int32, (RB, 8, 128), 0)
    system = sub % 4
    low = sub < 4

    def load(c):
        part = pl.ds(c * CHUNK, CHUNK)
        return pltpu.make_async_copy(tiles_hbm.at[part], raw.at[part], load_sem.at[c])

    small = [
        pltpu.make_async_copy(source, target, small_sem.at[i])
        for i, (source, target) in enumerate(
            ((req_hbm, req_ref), (b_hbm, b_ref), (row_hbm, row_s), (slot_hbm, slot_s))
        )
    ]
    small[0].start()
    barrier = pltpu.get_barrier_semaphore()
    for o in OFFSETS:
        pl.semaphore_signal(barrier, inc=1, device_id=(partner(o),), device_id_type=MESH)
    for copy in small[1:]:
        copy.start()
    for c in range(CHUNKS):
        load(c).start()
    small[0].wait()

    def split(v):
        hi = v.astype(BF16).astype(F32)
        return hi, v - hi

    def prepare(c, carry):
        load(c).wait()
        for i in range(CHUNK):
            t = raw[c * CHUNK + i].T
            hi = t.astype(BF16)
            lo = (t - hi.astype(F32)).astype(BF16)
            side = pl.ds((i % 2) * 128, 128)
            at = c * (CHUNK // 2) + i // 2
            wide[at, pl.ds(0, 128), side] = hi
            wide[at, pl.ds(128, 128), side] = lo
        return carry

    def start_send(phase, group, to, source, target):
        pltpu.make_async_remote_copy(
            src_ref=source, dst_ref=target.at[me], send_sem=send_sem.at[phase],
            recv_sem=recv_sem.at[phase, group], device_id=(to,), device_id_type=MESH,
        ).start()

    def wait_for(sem, like, count=N - 1):
        whole = like.at[pl.ds(0, count)]
        pltpu.make_async_copy(whole, whole, sem).wait()

    own_row = pltpu.make_async_copy(req_ref, ask_in.at[me], ask_sem)
    own_row.start()
    pl.semaphore_wait(barrier, N - 1)
    for o in OFFSETS:
        to = partner(o)
        start_send(0, 0, to, req_ref, ask_in)
    for copy in small[1:]:
        copy.wait()
    lax.fori_loop(0, CHUNKS, prepare, 0)

    def fold(v):
        return v + pltpu.roll(v, 4, 0)

    def product(u, v):
        s = fold(jnp.sum(u * v, axis=0))
        return jnp.broadcast_to(jnp.sum(s, axis=1, keepdims=True), (8, 128))

    def packed(values):
        y = jnp.zeros((8, 128), F32)
        for i, value in enumerate(values):
            y = jnp.where(lane // 16 == i, value, y)
        y = jnp.where((lane % 4 == sub), y, 0.0)
        return jnp.sum(y, axis=0, keepdims=True)

    def unpacked(total, count):
        spread = jnp.broadcast_to(total, (8, 128))
        out = []
        for i in range(count):
            picked = jnp.where(lane == i * 16 + system, spread, 0.0)
            out.append(jnp.broadcast_to(jnp.sum(picked, axis=1, keepdims=True), (8, 128)))
        return out

    def share(phase, partial):
        out, into = sums_out.at[phase], sums_in.at[phase]
        out[...] = partial
        into[me] = partial
        for o in OFFSETS:
            start_send(4 + phase, 0, partner(o), out, into)

    def gathered(phase):
        into = sums_in.at[phase]
        wait_for(recv_sem.at[4 + phase, 0], into)
        return jnp.sum(into[...], axis=0)

    def exchange(phase, vector):
        out, into = send.at[phase], got.at[phase]
        blocks = [vector[r // 2][r % 2 * 4 : r % 2 * 4 + 4] for r in range(RB)]
        for r in range(RB):
            staged[r] = blocks[r]
        targets = [partner(o) for o in BLOCKS] + [me]

        def fill(i):
            out[targets[i]] = staged[ask_in[targets[i], 0, me]]

        for i in range(ROWS_AHEAD):
            fill(i)
        for i, o in enumerate(BLOCKS):
            start_send(phase + 1, group_of(o), targets[i], out.at[targets[i]], into)
            if i + ROWS_AHEAD < N:
                fill(i + ROWS_AHEAD)
        into[me] = staged[ask_in[me, 0, me]]
        for r in range(RB):
            hi, lo = split(blocks[r])
            left[r] = jnp.concatenate([hi, lo], axis=0)

    def times(p, x0, x1):
        x = jnp.concatenate([x0, x1], axis=0).astype(BF16)
        x = jnp.concatenate([x, x], axis=1)
        r = jnp.dot(x, wide[p], preferred_element_type=F32)
        return r[0:8, 0:128], r[8:16, 128:256]

    def add(acc, row, value):
        return acc + jnp.where(block == row, value, 0.0)

    def own_tiles():
        acc = []
        for p in range(RB // 2):
            acc += times(p, left[2 * p], left[2 * p + 1])
        return jnp.stack(acc)

    def chip_tiles(into, offset, acc):
        first = partner(offset) - lax.rem(me, 2)
        x = []
        for d in (first, first + 1):
            hi, lo = split(into[d])
            x.append(jnp.concatenate([hi, lo], axis=0))
            left[RB + d] = x[-1]
        y0, y1 = times(RB // 2 + first // 2, x[0], x[1])
        return add(add(acc, row_s[RB + first], y0), row_s[RB + first + 1], y1)

    def extra_tiles(acc):
        for p in range(SLOTS // 2, PAIRS):
            y = times(p, left[slot_s[2 * p]], left[slot_s[2 * p + 1]])
            for t, value in ((2 * p, y[0]), (2 * p + 1, y[1])):
                acc = add(acc, jnp.where(t < count_s[0], row_s[t], -1), value)
        return acc

    def apply(phase, vector, partial, digest):
        exchange(phase, vector)
        share(phase, partial())
        into = got.at[phase]
        acc = own_tiles()
        for group in range(len(GROUPS)):
            wait_for(recv_sem.at[phase + 1, group], into, COUNTS[group])
            for offset in GROUPS[group]:
                acc = chip_tiles(into, offset, acc)
        acc = extra_tiles(acc)
        coefficients = digest(gathered(phase))
        acc = [fold(acc[r]) for r in range(RB)]
        z = jnp.stack([jnp.where(low, acc[2 * m], acc[2 * m + 1]) for m in range(RB // 2)])
        return coefficients, z

    b = b_ref[...]

    wait_for(recv_sem.at[0, 0], ask_in)
    own_row.wait()

    def digest0(total):
        (bb,) = unpacked(total, 1)
        beta = jnp.sqrt(bb + EPS)
        inverse = 1.0 / beta
        return beta, inverse, bb * inverse * inverse

    (beta, inverse, n00), z = apply(0, b, lambda: packed([product(b, b)]), digest0)
    v0 = b * inverse
    t1 = z * inverse

    def digest1(total):
        h00, tt = unpacked(total, 2)
        square = tt - 2.0 * h00 * h00 + h00 * h00 * n00
        guess1 = jnp.sqrt(jnp.maximum(square, 0.0) + EPS)
        return h00, guess1, 1.0 / guess1

    (h00, guess1, inverse), z = apply(1, t1, lambda: packed([product(t1, v0), product(t1, t1)]), digest1)
    u1 = (t1 - h00 * v0) * inverse
    t2 = (z - h00 * t1) * inverse

    def partial2():
        return packed(
            [product(t2, v0), product(t2, u1), product(t2, t2), product(u1, u1), product(u1, v0)]
        )

    def digest2(total):
        q0, q1, qq, m11, m01 = unpacked(total, 5)
        h10 = jnp.sqrt(guess1 * guess1 * m11 + EPS)
        rho = guess1 / h10
        d01 = rho * m01
        d11 = rho * rho * m11
        h01 = rho * q0
        x1 = rho * rho * q1
        h11 = x1 - h01 * d01
        square = (
            rho * rho * qq + h01 * h01 * n00 + h11 * h11 * d11
            - 2.0 * (h01 * h01 + h11 * x1) + 2.0 * h01 * h11 * d01
        )
        guess2 = jnp.sqrt(jnp.maximum(square, 0.0) + EPS)
        return h10, rho, d01, d11, h01, h11, guess2, 1.0 / guess2

    (h10, rho, d01, d11, h01, h11, guess2, inverse), z = apply(2, t2, partial2, digest2)
    v1 = u1 * rho
    s2 = t2 * rho
    u2 = (s2 - h01 * v0 - h11 * v1) * inverse
    t3 = (z * rho - h01 * t1 - h11 * s2) * inverse

    share(
        3,
        packed(
            [
                product(t3, v0), product(t3, v1), product(t3, u2), product(t3, t3),
                product(u2, u2), product(u2, v0), product(u2, v1),
            ]
        ),
    )

    def rotation(a, c):
        radius = jnp.sqrt(a * a + c * c)
        return a / radius, c / radius, radius

    c0, s0, r00 = rotation(h00, h10)
    g0, g1 = c0 * beta, -s0 * beta
    r01 = c0 * h01 + s0 * h11
    turned1 = c0 * h11 - s0 * h01

    p0, p1, p2, pp, m22, m02, m12 = unpacked(gathered(3), 7)
    h21 = jnp.sqrt(guess2 * guess2 * m22 + EPS)
    rho = guess2 / h21
    v2 = u2 * rho
    e02 = rho * m02
    e12 = rho * m12
    d22 = rho * rho * m22
    h02 = rho * p0
    x1 = rho * p1
    x2 = rho * rho * p2
    h12 = x1 - h02 * d01
    h22 = x2 - h02 * e02 - h12 * e12
    square = (
        rho * rho * pp + h02 * h02 * n00 + h12 * h12 * d11 + h22 * h22 * d22
        - 2.0 * (h02 * h02 + h12 * x1 + h22 * x2)
        + 2.0 * (h02 * h12 * d01 + h02 * h22 * e02 + h12 * h22 * e12)
    )
    h32 = jnp.sqrt(jnp.maximum(square, 0.0) + EPS)

    c1, s1, r11 = rotation(turned1, h21)
    g1, g2 = c1 * g1, -s1 * g1
    r02 = c0 * h02 + s0 * h12
    turned = c0 * h12 - s0 * h02
    r12 = c1 * turned + s1 * h22
    c2, s2, r22 = rotation(c1 * h22 - s1 * turned, h32)
    g2 = c2 * g2
    y2 = g2 / r22
    y1 = (g1 - r12 * y2) / r11
    y0 = (g0 - (r01 * y1 + r02 * y2)) / r00
    sol_ref[...] = y0 * v0 + y1 * v1 + y2 * v2

    columns = ((h00, h10), (h01, h11, h21), (h02, h12, h22, h32))
    for j, column in enumerate(columns):
        out = jnp.zeros((4, 4), F32)
        for i, value in enumerate(column):
            out = jnp.where(lane[0:4, 0:4] == i, value[0:4, 0:4], out)
        hes_ref[j] = out

    wait_for(send_sem.at[0], sums_in.at[0])
    for phase in range(3):
        wait_for(send_sem.at[phase + 1], send.at[phase])
    for phase in range(4):
        wait_for(send_sem.at[4 + phase], sums_in.at[phase])


def hand_over(answer_ref, hessenberg_ref, answer_out, hessenberg_out):
    answer_out[...] = answer_ref[...]
    hessenberg_out[...] = hessenberg_ref[...]


def solution(mesh):
    def on_device(tile_values, tile_row, tile_slot, tile_count, requests, right_side):
        vmem = pl.BlockSpec(memory_space=pltpu.VMEM)
        smem = pl.BlockSpec(memory_space=pltpu.SMEM)
        hbm = pl.BlockSpec(memory_space=pltpu.HBM)
        shapes = (
            jax.ShapeDtypeStruct((8, 8, 128), F32),
            jax.ShapeDtypeStruct((3, 4, 4), F32),
        )
        answer, hessenberg = pl.pallas_call(
            kernel,
            out_shape=shapes,
            in_specs=[smem, hbm, hbm, hbm, hbm, hbm],
            out_specs=(vmem, vmem),
            scratch_shapes=[
                pltpu.SMEM((TILES,), jnp.int32),
                pltpu.SMEM((TILES,), jnp.int32),
                pltpu.VMEM((1, 128), jnp.int32),
                pltpu.VMEM((8, 8, 128), F32),
                pltpu.VMEM((TILES, 128, 128), F32),
                pltpu.VMEM((PAIRS, 256, 256), BF16),
                pltpu.VMEM((SLOTS, 8, 128), F32),
                pltpu.VMEM((RB, 4, 128), F32),
                pltpu.VMEM((3, N, 4, 128), F32),
                pltpu.VMEM((3, N, 4, 128), F32),
                pltpu.SMEM((N, 1, 128), jnp.int32),
                pltpu.VMEM((4, 1, 128), F32),
                pltpu.VMEM((4, N, 1, 128), F32),
                pltpu.SemaphoreType.DMA((CHUNKS,)),
                pltpu.SemaphoreType.DMA((4,)),
                pltpu.SemaphoreType.DMA((8,)),
                pltpu.SemaphoreType.DMA((8, 2)),
                pltpu.SemaphoreType.DMA,
            ],
            compiler_params=pltpu.CompilerParams(
                collective_id=0, has_side_effects=True, vmem_limit_bytes=40 << 20
            ),
            name="arnoldi",
        )(
            tile_count,
            *[
                pltpu.with_memory_space_constraint(x, pltpu.HBM)
                for x in (
                    tile_row, tile_slot, tile_values,
                    requests.reshape(1, N), right_side.reshape(8, 8, 128),
                )
            ],
        )
        answer, hessenberg = pl.pallas_call(
            hand_over,
            out_shape=shapes,
            in_specs=[vmem, vmem],
            out_specs=(vmem, vmem),
            compiler_params=pltpu.CompilerParams(vmem_limit_bytes=4 << 20),
            name="hand_over",
        )(answer, hessenberg)
        return answer.reshape(RB, 4, 128), jnp.transpose(hessenberg, (1, 2, 0))

    rows = P("rows")
    return jax.shard_map(
        on_device,
        mesh=mesh,
        in_specs=(rows, rows, rows, rows, rows, rows),
        out_specs=(rows, P()),
        check_vma=False,
    )
```

```python
import jax
import jax.numpy as jnp
from jax import lax
from jax.experimental import pallas as pl
from jax.experimental.pallas import tpu as pltpu
from jax.sharding import PartitionSpec as P

MESH = pl.DeviceIdType.MESH
F32 = jnp.float32
BF16 = jnp.bfloat16
EPS = 1e-06
N = 128
RB = 16
TILES = 208
SLOTS = 144
PAIRS = TILES // 2
CHUNK = 16
CHUNKS = TILES // CHUNK
ROWS_AHEAD = 12


def hops(offset):
    return sum(min(d, 4 - d) for d in ((offset // 2) % 4, (offset // 8) % 4, offset // 32))


OFFSETS = sorted(range(1, N), key=lambda o: (-hops(o), o))
BLOCK_ORDER = (6, 5, 4, 3, 2, 1, 0)
BLOCKS = sorted(range(1, N), key=lambda o: (BLOCK_ORDER.index(hops(o)), o))
GROUP_HOPS = ((4, 5, 6), (0, 1, 2, 3))
GROUPS = [[o for o in range(0, N, 2) if hops(o) in group] for group in GROUP_HOPS]
COUNTS = [sum(hops(o) in group for o in OFFSETS) for group in GROUP_HOPS]


def group_of(o):
    return [i for i, group in enumerate(GROUP_HOPS) if hops(o) in group][0]


def partners(me):
    def turned(step, size):
        digit = lax.rem(lax.div(me, step), size)
        return [lax.rem(digit + k, size) * step for k in range(size)]

    cores, y, z, x = turned(1, 2), turned(2, 4), turned(8, 4), turned(32, 4)
    return lambda o: cores[o % 2] + (y[o // 2 % 4] + (z[o // 8 % 4] + x[o // 32]))


def kernel(
    count_s, row_hbm, slot_hbm, tiles_hbm, req_hbm, b_hbm,
    sol_ref, hes_ref,
    row_s, slot_s, req_ref, b_ref,
    raw, wide, left, staged, send, got, ask_in, sums_out, sums_in,
    load_sem, small_sem, send_sem, recv_sem, ask_sem,
):
    me = lax.axis_index("rows")
    partner = partners(me)
    lane = lax.broadcasted_iota(jnp.int32, (8, 128), 1)
    sub = lax.broadcasted_iota(jnp.int32, (8, 128), 0)
    block = lax.broadcasted_iota(jnp.int32, (RB, 8, 128), 0)
    system = sub % 4
    low = sub < 4

    def load(c):
        part = pl.ds(c * CHUNK, CHUNK)
        return pltpu.make_async_copy(tiles_hbm.at[part], raw.at[part], load_sem.at[c])

    small = [
        pltpu.make_async_copy(source, target, small_sem.at[i])
        for i, (source, target) in enumerate(
            ((req_hbm, req_ref), (b_hbm, b_ref), (row_hbm, row_s), (slot_hbm, slot_s))
        )
    ]
    small[0].start()
    barrier = pltpu.get_barrier_semaphore()
    for o in OFFSETS:
        pl.semaphore_signal(barrier, inc=1, device_id=(partner(o),), device_id_type=MESH)
    for copy in small[1:]:
        copy.start()
    for c in range(CHUNKS):
        load(c).start()
    small[0].wait()

    def split(v):
        hi = v.astype(BF16).astype(F32)
        return hi, v - hi

    def prepare(c, carry):
        load(c).wait()
        for i in range(CHUNK):
            t = raw[c * CHUNK + i].T
            hi = t.astype(BF16)
            lo = (t - hi.astype(F32)).astype(BF16)
            side = pl.ds((i % 2) * 128, 128)
            at = c * (CHUNK // 2) + i // 2
            wide[at, pl.ds(0, 128), side] = hi
            wide[at, pl.ds(128, 128), side] = lo
        return carry

    def start_send(phase, group, to, source, target):
        pltpu.make_async_remote_copy(
            src_ref=source, dst_ref=target.at[me], send_sem=send_sem.at[phase],
            recv_sem=recv_sem.at[phase, group], device_id=(to,), device_id_type=MESH,
        ).start()

    def wait_for(sem, like, count=N - 1):
        whole = like.at[pl.ds(0, count)]
        pltpu.make_async_copy(whole, whole, sem).wait()

    own_row = pltpu.make_async_copy(req_ref, ask_in.at[me], ask_sem)
    own_row.start()
    pl.semaphore_wait(barrier, N - 1)
    for o in OFFSETS:
        to = partner(o)
        start_send(0, 0, to, req_ref, ask_in)
    for copy in small[1:]:
        copy.wait()
    lax.fori_loop(0, CHUNKS, prepare, 0)

    def fold(v):
        return v + pltpu.roll(v, 4, 0)

    def product(u, v):
        s = fold(jnp.sum(u * v, axis=0))
        return jnp.broadcast_to(jnp.sum(s, axis=1, keepdims=True), (8, 128))

    def packed(values):
        y = jnp.zeros((8, 128), F32)
        for i, value in enumerate(values):
            y = jnp.where(lane // 16 == i, value, y)
        y = jnp.where((lane % 4 == sub), y, 0.0)
        return jnp.sum(y, axis=0, keepdims=True)

    def unpacked(total, count):
        spread = jnp.broadcast_to(total, (8, 128))
        out = []
        for i in range(count):
            picked = jnp.where(lane == i * 16 + system, spread, 0.0)
            out.append(jnp.broadcast_to(jnp.sum(picked, axis=1, keepdims=True), (8, 128)))
        return out

    def share(phase, partial):
        out, into = sums_out.at[phase], sums_in.at[phase]
        out[...] = partial
        into[me] = partial
        for o in OFFSETS:
            start_send(4 + phase, 0, partner(o), out, into)

    def gathered(phase):
        into = sums_in.at[phase]
        wait_for(recv_sem.at[4 + phase, 0], into)
        quarters = [jnp.sum(into[pl.ds(i * 32, 32)], axis=0) for i in range(4)]
        return (quarters[0] + quarters[1]) + (quarters[2] + quarters[3])

    def exchange(phase, vector):
        out, into = send.at[phase], got.at[phase]
        blocks = [vector[r // 2][r % 2 * 4 : r % 2 * 4 + 4] for r in range(RB)]
        for r in range(RB):
            staged[r] = blocks[r]
        targets = [partner(o) for o in BLOCKS] + [me]

        def fill(i):
            out[targets[i]] = staged[ask_in[targets[i], 0, me]]

        for i in range(ROWS_AHEAD):
            fill(i)
        for i, o in enumerate(BLOCKS):
            start_send(phase + 1, group_of(o), targets[i], out.at[targets[i]], into)
            if i + ROWS_AHEAD < N:
                fill(i + ROWS_AHEAD)
        into[me] = staged[ask_in[me, 0, me]]
        for r in range(RB):
            hi, lo = split(blocks[r])
            left[r] = jnp.concatenate([hi, lo], axis=0)

    def times(p, x0, x1):
        x = jnp.concatenate([x0, x1], axis=0).astype(BF16)
        x = jnp.concatenate([x, x], axis=1)
        r = jnp.dot(x, wide[p], preferred_element_type=F32)
        return r[0:8, 0:128], r[8:16, 128:256]

    def add(acc, row, value):
        return acc + jnp.where(block == row, value, 0.0)

    def own_tiles():
        acc = []
        for p in range(RB // 2):
            acc += times(p, left[2 * p], left[2 * p + 1])
        return jnp.stack(acc)

    def chip_tiles(into, offset, acc):
        first = partner(offset) - lax.rem(me, 2)
        x = []
        for d in (first, first + 1):
            hi, lo = split(into[d])
            x.append(jnp.concatenate([hi, lo], axis=0))
            left[RB + d] = x[-1]
        y0, y1 = times(RB // 2 + first // 2, x[0], x[1])
        return add(add(acc, row_s[RB + first], y0), row_s[RB + first + 1], y1)

    def extra_tiles(acc):
        for p in range(SLOTS // 2, PAIRS):
            y = times(p, left[slot_s[2 * p]], left[slot_s[2 * p + 1]])
            for t, value in ((2 * p, y[0]), (2 * p + 1, y[1])):
                acc = add(acc, jnp.where(t < count_s[0], row_s[t], -1), value)
        return acc

    def apply(phase, vector, partial, digest):
        exchange(phase, vector)
        share(phase, partial())
        into = got.at[phase]
        acc = own_tiles()
        for group in range(len(GROUPS)):
            wait_for(recv_sem.at[phase + 1, group], into, COUNTS[group])
            for offset in GROUPS[group]:
                acc = chip_tiles(into, offset, acc)
        acc = extra_tiles(acc)
        coefficients = digest(gathered(phase))
        acc = [fold(acc[r]) for r in range(RB)]
        z = jnp.stack([jnp.where(low, acc[2 * m], acc[2 * m + 1]) for m in range(RB // 2)])
        return coefficients, z

    b = b_ref[...]

    wait_for(recv_sem.at[0, 0], ask_in)
    own_row.wait()

    def digest0(total):
        (bb,) = unpacked(total, 1)
        beta = jnp.sqrt(bb + EPS)
        inverse = 1.0 / beta
        return beta, inverse, bb * inverse * inverse

    (beta, inverse, n00), z = apply(0, b, lambda: packed([product(b, b)]), digest0)
    v0 = b * inverse
    t1 = z * inverse

    def digest1(total):
        h00, tt = unpacked(total, 2)
        square = tt - 2.0 * h00 * h00 + h00 * h00 * n00
        guess1 = jnp.sqrt(jnp.maximum(square, 0.0) + EPS)
        return h00, guess1, 1.0 / guess1

    (h00, guess1, inverse), z = apply(1, t1, lambda: packed([product(t1, v0), product(t1, t1)]), digest1)
    u1 = (t1 - h00 * v0) * inverse
    t2 = (z - h00 * t1) * inverse

    def partial2():
        return packed(
            [product(t2, v0), product(t2, u1), product(t2, t2), product(u1, u1), product(u1, v0)]
        )

    def digest2(total):
        q0, q1, qq, m11, m01 = unpacked(total, 5)
        h10 = jnp.sqrt(guess1 * guess1 * m11 + EPS)
        rho = guess1 / h10
        d01 = rho * m01
        d11 = rho * rho * m11
        h01 = rho * q0
        x1 = rho * rho * q1
        h11 = x1 - h01 * d01
        square = (
            rho * rho * qq + h01 * h01 * n00 + h11 * h11 * d11
            - 2.0 * (h01 * h01 + h11 * x1) + 2.0 * h01 * h11 * d01
        )
        guess2 = jnp.sqrt(jnp.maximum(square, 0.0) + EPS)
        return h10, rho, d01, d11, h01, h11, guess2, 1.0 / guess2

    (h10, rho, d01, d11, h01, h11, guess2, inverse), z = apply(2, t2, partial2, digest2)
    v1 = u1 * rho
    s2 = t2 * rho
    u2 = (s2 - h01 * v0 - h11 * v1) * inverse
    t3 = (z * rho - h01 * t1 - h11 * s2) * inverse

    share(
        3,
        packed(
            [
                product(t3, v0), product(t3, v1), product(t3, u2), product(t3, t3),
                product(u2, u2), product(u2, v0), product(u2, v1),
            ]
        ),
    )

    def rotation(a, c):
        radius = jnp.sqrt(a * a + c * c)
        return a / radius, c / radius, radius

    c0, s0, r00 = rotation(h00, h10)
    g0, g1 = c0 * beta, -s0 * beta
    r01 = c0 * h01 + s0 * h11
    turned1 = c0 * h11 - s0 * h01

    p0, p1, p2, pp, m22, m02, m12 = unpacked(gathered(3), 7)
    h21 = jnp.sqrt(guess2 * guess2 * m22 + EPS)
    rho = guess2 / h21
    v2 = u2 * rho
    e02 = rho * m02
    e12 = rho * m12
    d22 = rho * rho * m22
    h02 = rho * p0
    x1 = rho * p1
    x2 = rho * rho * p2
    h12 = x1 - h02 * d01
    h22 = x2 - h02 * e02 - h12 * e12
    square = (
        rho * rho * pp + h02 * h02 * n00 + h12 * h12 * d11 + h22 * h22 * d22
        - 2.0 * (h02 * h02 + h12 * x1 + h22 * x2)
        + 2.0 * (h02 * h12 * d01 + h02 * h22 * e02 + h12 * h22 * e12)
    )
    h32 = jnp.sqrt(jnp.maximum(square, 0.0) + EPS)

    c1, s1, r11 = rotation(turned1, h21)
    g1, g2 = c1 * g1, -s1 * g1
    r02 = c0 * h02 + s0 * h12
    turned = c0 * h12 - s0 * h02
    r12 = c1 * turned + s1 * h22
    c2, s2, r22 = rotation(c1 * h22 - s1 * turned, h32)
    g2 = c2 * g2
    y2 = g2 / r22
    y1 = (g1 - r12 * y2) / r11
    y0 = (g0 - (r01 * y1 + r02 * y2)) / r00
    sol_ref[...] = y0 * v0 + y1 * v1 + y2 * v2

    columns = ((h00, h10), (h01, h11, h21), (h02, h12, h22, h32))
    for j, column in enumerate(columns):
        out = jnp.zeros((4, 4), F32)
        for i, value in enumerate(column):
            out = jnp.where(lane[0:4, 0:4] == i, value[0:4, 0:4], out)
        hes_ref[j] = out

    wait_for(send_sem.at[0], sums_in.at[0])
    for phase in range(3):
        wait_for(send_sem.at[phase + 1], send.at[phase])
    for phase in range(4):
        wait_for(send_sem.at[4 + phase], sums_in.at[phase])


def hand_over(answer_ref, hessenberg_ref, answer_out, hessenberg_out):
    answer_out[...] = answer_ref[...]
    hessenberg_out[...] = hessenberg_ref[...]


def solution(mesh):
    def on_device(tile_values, tile_row, tile_slot, tile_count, requests, right_side):
        vmem = pl.BlockSpec(memory_space=pltpu.VMEM)
        smem = pl.BlockSpec(memory_space=pltpu.SMEM)
        hbm = pl.BlockSpec(memory_space=pltpu.HBM)
        shapes = (
            jax.ShapeDtypeStruct((8, 8, 128), F32),
            jax.ShapeDtypeStruct((3, 4, 4), F32),
        )
        answer, hessenberg = pl.pallas_call(
            kernel,
            out_shape=shapes,
            in_specs=[smem, hbm, hbm, hbm, hbm, hbm],
            out_specs=(vmem, vmem),
            scratch_shapes=[
                pltpu.SMEM((TILES,), jnp.int32),
                pltpu.SMEM((TILES,), jnp.int32),
                pltpu.VMEM((1, 128), jnp.int32),
                pltpu.VMEM((8, 8, 128), F32),
                pltpu.VMEM((TILES, 128, 128), F32),
                pltpu.VMEM((PAIRS, 256, 256), BF16),
                pltpu.VMEM((SLOTS, 8, 128), F32),
                pltpu.VMEM((RB, 4, 128), F32),
                pltpu.VMEM((3, N, 4, 128), F32),
                pltpu.VMEM((3, N, 4, 128), F32),
                pltpu.SMEM((N, 1, 128), jnp.int32),
                pltpu.VMEM((4, 1, 128), F32),
                pltpu.VMEM((4, N, 1, 128), F32),
                pltpu.SemaphoreType.DMA((CHUNKS,)),
                pltpu.SemaphoreType.DMA((4,)),
                pltpu.SemaphoreType.DMA((8,)),
                pltpu.SemaphoreType.DMA((8, 2)),
                pltpu.SemaphoreType.DMA,
            ],
            compiler_params=pltpu.CompilerParams(
                collective_id=0, has_side_effects=True, vmem_limit_bytes=40 << 20
            ),
            name="arnoldi",
        )(
            tile_count,
            *[
                pltpu.with_memory_space_constraint(x, pltpu.HBM)
                for x in (
                    tile_row, tile_slot, tile_values,
                    requests.reshape(1, N), right_side.reshape(8, 8, 128),
                )
            ],
        )
        answer, hessenberg = pl.pallas_call(
            hand_over,
            out_shape=shapes,
            in_specs=[vmem, vmem],
            out_specs=(vmem, vmem),
            compiler_params=pltpu.CompilerParams(vmem_limit_bytes=4 << 20),
            name="hand_over",
        )(answer, hessenberg)
        return answer.reshape(RB, 4, 128), jnp.transpose(hessenberg, (1, 2, 0))

    rows = P("rows")
    return jax.shard_map(
        on_device,
        mesh=mesh,
        in_specs=(rows, rows, rows, rows, rows, rows),
        out_specs=(rows, P()),
        check_vma=False,
    )
```

```python
import jax
import jax.numpy as jnp
from jax import lax
from jax.experimental import pallas as pl
from jax.experimental.pallas import tpu as pltpu
from jax.sharding import PartitionSpec as P

MESH = pl.DeviceIdType.MESH
F32 = jnp.float32
BF16 = jnp.bfloat16
EPS = 1e-06
N = 128
RB = 16
TILES = 208
SLOTS = 144
PAIRS = TILES // 2
CHUNK = 16
CHUNKS = TILES // CHUNK
ROWS_AHEAD = 12


def hops(offset):
    return sum(min(d, 4 - d) for d in ((offset // 2) % 4, (offset // 8) % 4, offset // 32))


OFFSETS = sorted(range(1, N), key=lambda o: (-hops(o), o))
BLOCK_ORDER = (6, 5, 4, 3, 2, 1, 0)
BLOCKS = sorted(range(1, N), key=lambda o: (BLOCK_ORDER.index(hops(o)), o))
GROUP_HOPS = ((4, 5, 6), (0, 1, 2, 3))
GROUPS = [[o for o in range(0, N, 2) if hops(o) in group] for group in GROUP_HOPS]
COUNTS = [sum(hops(o) in group for o in OFFSETS) for group in GROUP_HOPS]


def group_of(o):
    return [i for i, group in enumerate(GROUP_HOPS) if hops(o) in group][0]


def partners(me):
    def turned(step, size):
        digit = lax.rem(lax.div(me, step), size)
        return [lax.rem(digit + k, size) * step for k in range(size)]

    cores, y, z, x = turned(1, 2), turned(2, 4), turned(8, 4), turned(32, 4)
    return lambda o: cores[o % 2] + (y[o // 2 % 4] + (z[o // 8 % 4] + x[o // 32]))


def kernel(
    count_s, row_hbm, slot_hbm, tiles_hbm, req_hbm, b_hbm,
    sol_ref, hes_ref,
    row_s, slot_s, req_ref, b_ref,
    raw, wide, left, staged, send, got, ask_in, sums_out, sums_in, mate_out, mate_in,
    load_sem, small_sem, send_sem, recv_sem, ask_sem, mate_sem,
):
    me = lax.axis_index("rows")
    partner = partners(me)
    lane = lax.broadcasted_iota(jnp.int32, (8, 128), 1)
    sub = lax.broadcasted_iota(jnp.int32, (8, 128), 0)
    block = lax.broadcasted_iota(jnp.int32, (RB, 8, 128), 0)
    system = sub % 4
    low = sub < 4

    def load(c):
        part = pl.ds(c * CHUNK, CHUNK)
        return pltpu.make_async_copy(tiles_hbm.at[part], raw.at[part], load_sem.at[c])

    small = [
        pltpu.make_async_copy(source, target, small_sem.at[i])
        for i, (source, target) in enumerate(
            ((req_hbm, req_ref), (b_hbm, b_ref), (row_hbm, row_s), (slot_hbm, slot_s))
        )
    ]
    small[0].start()
    barrier = pltpu.get_barrier_semaphore()
    for o in OFFSETS:
        pl.semaphore_signal(barrier, inc=1, device_id=(partner(o),), device_id_type=MESH)
    for copy in small[1:]:
        copy.start()
    for c in range(CHUNKS):
        load(c).start()
    small[0].wait()

    def split(v):
        hi = v.astype(BF16).astype(F32)
        return hi, v - hi

    def prepare(c, carry):
        load(c).wait()
        for i in range(CHUNK):
            t = raw[c * CHUNK + i].T
            hi = t.astype(BF16)
            lo = (t - hi.astype(F32)).astype(BF16)
            side = pl.ds((i % 2) * 128, 128)
            at = c * (CHUNK // 2) + i // 2
            wide[at, pl.ds(0, 128), side] = hi
            wide[at, pl.ds(128, 128), side] = lo
        return carry

    def start_send(phase, group, to, source, target):
        pltpu.make_async_remote_copy(
            src_ref=source, dst_ref=target.at[me], send_sem=send_sem.at[phase],
            recv_sem=recv_sem.at[phase, group], device_id=(to,), device_id_type=MESH,
        ).start()

    def wait_for(sem, like, count=N - 1):
        whole = like.at[pl.ds(0, count)]
        pltpu.make_async_copy(whole, whole, sem).wait()

    own_row = pltpu.make_async_copy(req_ref, ask_in.at[me], ask_sem)
    own_row.start()
    pl.semaphore_wait(barrier, N - 1)
    for o in OFFSETS:
        to = partner(o)
        start_send(0, 0, to, req_ref, ask_in)
    for copy in small[1:]:
        copy.wait()
    lax.fori_loop(0, CHUNKS, prepare, 0)

    def fold(v):
        return v + pltpu.roll(v, 4, 0)

    def product(u, v):
        s = fold(jnp.sum(u * v, axis=0))
        return jnp.broadcast_to(jnp.sum(s, axis=1, keepdims=True), (8, 128))

    def packed(values):
        y = jnp.zeros((8, 128), F32)
        for i, value in enumerate(values):
            y = jnp.where(lane // 16 == i, value, y)
        y = jnp.where((lane % 4 == sub), y, 0.0)
        return jnp.sum(y, axis=0, keepdims=True)

    def unpacked(total, count):
        spread = jnp.broadcast_to(total, (8, 128))
        out = []
        for i in range(count):
            picked = jnp.where(lane == i * 16 + system, spread, 0.0)
            out.append(jnp.broadcast_to(jnp.sum(picked, axis=1, keepdims=True), (8, 128)))
        return out

    def share_by_chip(phase, partial):
        mate = partner(1)
        own_out, own_in = mate_out.at[phase], mate_in.at[phase]
        own_out[...] = partial
        hand = pltpu.make_async_remote_copy(
            src_ref=own_out, dst_ref=own_in, send_sem=mate_sem.at[phase, 0],
            recv_sem=mate_sem.at[phase, 1], device_id=(mate,), device_id_type=MESH,
        )
        hand.start()
        acc = own_tiles()
        hand.wait()
        both = partial + own_in[...]
        out, into = sums_out.at[phase], sums_in.at[phase]
        out[...] = both
        chip = lax.div(me, 2)
        into[chip] = both
        for o in OFFSETS:
            if o % 2 == 0:
                pltpu.make_async_remote_copy(
                    src_ref=out, dst_ref=into.at[chip], send_sem=send_sem.at[4 + phase],
                    recv_sem=recv_sem.at[4 + phase, 0], device_id=(partner(o),), device_id_type=MESH,
                ).start()
        return acc

    def gathered_by_chip(phase):
        into = sums_in.at[phase]
        wait_for(recv_sem.at[4 + phase, 0], into, N // 2 - 1)
        quarters = [jnp.sum(into[pl.ds(i * 16, 16)], axis=0) for i in range(4)]
        return (quarters[0] + quarters[1]) + (quarters[2] + quarters[3])

    def share(phase, partial):
        out, into = sums_out.at[phase], sums_in.at[phase]
        out[...] = partial
        into[me] = partial
        for o in OFFSETS:
            start_send(4 + phase, 0, partner(o), out, into)

    def gathered(phase):
        into = sums_in.at[phase]
        wait_for(recv_sem.at[4 + phase, 0], into)
        quarters = [jnp.sum(into[pl.ds(i * 32, 32)], axis=0) for i in range(4)]
        return (quarters[0] + quarters[1]) + (quarters[2] + quarters[3])

    def exchange(phase, vector):
        out, into = send.at[phase], got.at[phase]
        blocks = [vector[r // 2][r % 2 * 4 : r % 2 * 4 + 4] for r in range(RB)]
        for r in range(RB):
            staged[r] = blocks[r]
        targets = [partner(o) for o in BLOCKS] + [me]

        def fill(i):
            out[targets[i]] = staged[ask_in[targets[i], 0, me]]

        for i in range(ROWS_AHEAD):
            fill(i)
        for i, o in enumerate(BLOCKS):
            start_send(phase + 1, group_of(o), targets[i], out.at[targets[i]], into)
            if i + ROWS_AHEAD < N:
                fill(i + ROWS_AHEAD)
        into[me] = staged[ask_in[me, 0, me]]
        for r in range(RB):
            hi, lo = split(blocks[r])
            left[r] = jnp.concatenate([hi, lo], axis=0)

    def times(p, x0, x1):
        x = jnp.concatenate([x0, x1], axis=0).astype(BF16)
        x = jnp.concatenate([x, x], axis=1)
        r = jnp.dot(x, wide[p], preferred_element_type=F32)
        return r[0:8, 0:128], r[8:16, 128:256]

    def add(acc, row, value):
        return acc + jnp.where(block == row, value, 0.0)

    def own_tiles():
        acc = []
        for p in range(RB // 2):
            acc += times(p, left[2 * p], left[2 * p + 1])
        return jnp.stack(acc)

    def chip_tiles(into, offset, acc):
        first = partner(offset) - lax.rem(me, 2)
        x = []
        for d in (first, first + 1):
            hi, lo = split(into[d])
            x.append(jnp.concatenate([hi, lo], axis=0))
            left[RB + d] = x[-1]
        y0, y1 = times(RB // 2 + first // 2, x[0], x[1])
        return add(add(acc, row_s[RB + first], y0), row_s[RB + first + 1], y1)

    def extra_tiles(acc):
        for p in range(SLOTS // 2, PAIRS):
            y = times(p, left[slot_s[2 * p]], left[slot_s[2 * p + 1]])
            for t, value in ((2 * p, y[0]), (2 * p + 1, y[1])):
                acc = add(acc, jnp.where(t < count_s[0], row_s[t], -1), value)
        return acc

    def apply(phase, vector, partial, digest):
        exchange(phase, vector)
        acc = share_by_chip(phase, partial())
        into = got.at[phase]
        for group in range(len(GROUPS)):
            wait_for(recv_sem.at[phase + 1, group], into, COUNTS[group])
            for offset in GROUPS[group]:
                acc = chip_tiles(into, offset, acc)
        acc = extra_tiles(acc)
        coefficients = digest(gathered_by_chip(phase))
        acc = [fold(acc[r]) for r in range(RB)]
        z = jnp.stack([jnp.where(low, acc[2 * m], acc[2 * m + 1]) for m in range(RB // 2)])
        return coefficients, z

    b = b_ref[...]

    wait_for(recv_sem.at[0, 0], ask_in)
    own_row.wait()

    def digest0(total):
        (bb,) = unpacked(total, 1)
        beta = jnp.sqrt(bb + EPS)
        inverse = 1.0 / beta
        return beta, inverse, bb * inverse * inverse

    (beta, inverse, n00), z = apply(0, b, lambda: packed([product(b, b)]), digest0)
    v0 = b * inverse
    t1 = z * inverse

    def digest1(total):
        h00, tt = unpacked(total, 2)
        square = tt - 2.0 * h00 * h00 + h00 * h00 * n00
        guess1 = jnp.sqrt(jnp.maximum(square, 0.0) + EPS)
        return h00, guess1, 1.0 / guess1

    (h00, guess1, inverse), z = apply(1, t1, lambda: packed([product(t1, v0), product(t1, t1)]), digest1)
    u1 = (t1 - h00 * v0) * inverse
    t2 = (z - h00 * t1) * inverse

    def partial2():
        return packed(
            [product(t2, v0), product(t2, u1), product(t2, t2), product(u1, u1), product(u1, v0)]
        )

    def digest2(total):
        q0, q1, qq, m11, m01 = unpacked(total, 5)
        h10 = jnp.sqrt(guess1 * guess1 * m11 + EPS)
        rho = guess1 / h10
        d01 = rho * m01
        d11 = rho * rho * m11
        h01 = rho * q0
        x1 = rho * rho * q1
        h11 = x1 - h01 * d01
        square = (
            rho * rho * qq + h01 * h01 * n00 + h11 * h11 * d11
            - 2.0 * (h01 * h01 + h11 * x1) + 2.0 * h01 * h11 * d01
        )
        guess2 = jnp.sqrt(jnp.maximum(square, 0.0) + EPS)
        return h10, rho, d01, d11, h01, h11, guess2, 1.0 / guess2

    (h10, rho, d01, d11, h01, h11, guess2, inverse), z = apply(2, t2, partial2, digest2)
    v1 = u1 * rho
    s2 = t2 * rho
    u2 = (s2 - h01 * v0 - h11 * v1) * inverse
    t3 = (z * rho - h01 * t1 - h11 * s2) * inverse

    share(
        3,
        packed(
            [
                product(t3, v0), product(t3, v1), product(t3, u2), product(t3, t3),
                product(u2, u2), product(u2, v0), product(u2, v1),
            ]
        ),
    )

    def rotation(a, c):
        radius = jnp.sqrt(a * a + c * c)
        return a / radius, c / radius, radius

    c0, s0, r00 = rotation(h00, h10)
    g0, g1 = c0 * beta, -s0 * beta
    r01 = c0 * h01 + s0 * h11
    turned1 = c0 * h11 - s0 * h01

    p0, p1, p2, pp, m22, m02, m12 = unpacked(gathered(3), 7)
    h21 = jnp.sqrt(guess2 * guess2 * m22 + EPS)
    rho = guess2 / h21
    v2 = u2 * rho
    e02 = rho * m02
    e12 = rho * m12
    d22 = rho * rho * m22
    h02 = rho * p0
    x1 = rho * p1
    x2 = rho * rho * p2
    h12 = x1 - h02 * d01
    h22 = x2 - h02 * e02 - h12 * e12
    square = (
        rho * rho * pp + h02 * h02 * n00 + h12 * h12 * d11 + h22 * h22 * d22
        - 2.0 * (h02 * h02 + h12 * x1 + h22 * x2)
        + 2.0 * (h02 * h12 * d01 + h02 * h22 * e02 + h12 * h22 * e12)
    )
    h32 = jnp.sqrt(jnp.maximum(square, 0.0) + EPS)

    c1, s1, r11 = rotation(turned1, h21)
    g1, g2 = c1 * g1, -s1 * g1
    r02 = c0 * h02 + s0 * h12
    turned = c0 * h12 - s0 * h02
    r12 = c1 * turned + s1 * h22
    c2, s2, r22 = rotation(c1 * h22 - s1 * turned, h32)
    g2 = c2 * g2
    y2 = g2 / r22
    y1 = (g1 - r12 * y2) / r11
    y0 = (g0 - (r01 * y1 + r02 * y2)) / r00
    sol_ref[...] = y0 * v0 + y1 * v1 + y2 * v2

    columns = ((h00, h10), (h01, h11, h21), (h02, h12, h22, h32))
    for j, column in enumerate(columns):
        out = jnp.zeros((4, 4), F32)
        for i, value in enumerate(column):
            out = jnp.where(lane[0:4, 0:4] == i, value[0:4, 0:4], out)
        hes_ref[j] = out

    wait_for(send_sem.at[0], sums_in.at[0])
    for phase in range(3):
        wait_for(send_sem.at[phase + 1], send.at[phase])
    for phase in range(4):
        wait_for(send_sem.at[4 + phase], sums_in.at[phase], N - 1 if phase == 3 else N // 2 - 1)


def hand_over(answer_ref, hessenberg_ref, answer_out, hessenberg_out):
    answer_out[...] = answer_ref[...]
    hessenberg_out[...] = hessenberg_ref[...]


def solution(mesh):
    def on_device(tile_values, tile_row, tile_slot, tile_count, requests, right_side):
        vmem = pl.BlockSpec(memory_space=pltpu.VMEM)
        smem = pl.BlockSpec(memory_space=pltpu.SMEM)
        hbm = pl.BlockSpec(memory_space=pltpu.HBM)
        shapes = (
            jax.ShapeDtypeStruct((8, 8, 128), F32),
            jax.ShapeDtypeStruct((3, 4, 4), F32),
        )
        answer, hessenberg = pl.pallas_call(
            kernel,
            out_shape=shapes,
            in_specs=[smem, hbm, hbm, hbm, hbm, hbm],
            out_specs=(vmem, vmem),
            scratch_shapes=[
                pltpu.SMEM((TILES,), jnp.int32),
                pltpu.SMEM((TILES,), jnp.int32),
                pltpu.VMEM((1, 128), jnp.int32),
                pltpu.VMEM((8, 8, 128), F32),
                pltpu.VMEM((TILES, 128, 128), F32),
                pltpu.VMEM((PAIRS, 256, 256), BF16),
                pltpu.VMEM((SLOTS, 8, 128), F32),
                pltpu.VMEM((RB, 4, 128), F32),
                pltpu.VMEM((3, N, 4, 128), F32),
                pltpu.VMEM((3, N, 4, 128), F32),
                pltpu.SMEM((N, 1, 128), jnp.int32),
                pltpu.VMEM((4, 1, 128), F32),
                pltpu.VMEM((4, N, 1, 128), F32),
                pltpu.VMEM((3, 1, 128), F32),
                pltpu.VMEM((3, 1, 128), F32),
                pltpu.SemaphoreType.DMA((CHUNKS,)),
                pltpu.SemaphoreType.DMA((4,)),
                pltpu.SemaphoreType.DMA((8,)),
                pltpu.SemaphoreType.DMA((8, 2)),
                pltpu.SemaphoreType.DMA,
                pltpu.SemaphoreType.DMA((3, 2)),
            ],
            compiler_params=pltpu.CompilerParams(
                collective_id=0, has_side_effects=True, vmem_limit_bytes=40 << 20
            ),
            name="arnoldi",
        )(
            tile_count,
            *[
                pltpu.with_memory_space_constraint(x, pltpu.HBM)
                for x in (
                    tile_row, tile_slot, tile_values,
                    requests.reshape(1, N), right_side.reshape(8, 8, 128),
                )
            ],
        )
        answer, hessenberg = pl.pallas_call(
            hand_over,
            out_shape=shapes,
            in_specs=[vmem, vmem],
            out_specs=(vmem, vmem),
            compiler_params=pltpu.CompilerParams(vmem_limit_bytes=4 << 20),
            name="hand_over",
        )(answer, hessenberg)
        return answer.reshape(RB, 4, 128), jnp.transpose(hessenberg, (1, 2, 0))

    rows = P("rows")
    return jax.shard_map(
        on_device,
        mesh=mesh,
        in_specs=(rows, rows, rows, rows, rows, rows),
        out_specs=(rows, P()),
        check_vma=False,
    )
```
